32 devices in a mesh: prow: 4 (over z), pcol: 8 (over y, x, core).
Axes of the slice: x: 2, y: 2, z: 4, core: 2. Of those that a mesh axis runs over, the one named last changes fastest.
Arguments:
- values: float32 [12, 4, 4, 8, 256, 256], P(None, 'prow', None, 'pcol'), may hold values from -6 to 6
- pattern: int32 [12, 4, 4, 8], P(None, 'prow', None, 'pcol'), may hold values from 0 to 1
Outputs:
- factored: float32 [12, 4, 4, 8, 256, 256], P(None, 'prow', None, 'pcol')
The draws below stay inside these ranges and needn't reach their ends.
All inputs are finite; a program needn't handle non-finite values.
Results may differ from the reference program's by a relative error of at most 0.0003.
Values sent between devices are 32-bit elements; how exact they have to be, the bound alone decides.
No kernel may reach another device: no remote copies, remote signals or barrier semaphores. Data moves between devices by JAX's collectives and lax.ppermute only.
A program may use at most 128 MiB of HBM per device.

```python
import math
import jax
import jax.numpy as jnp
from jax import lax

B = 256
LR = 12
LC = 4
SWEEPS = 3
N_PROW = 4
N_PCOL = 8


def draw_values(key, part):
    shape = (LR, N_PROW, LC, N_PCOL, B, B)
    return jnp.clip(jax.random.normal(jax.random.fold_in(key, 7), shape, jnp.float32), -6.0, 6.0)


def touch_ends(drawn, rng, low, top_value):
    place = [jax.random.randint(jax.random.fold_in(rng, axis), (), 0, length) for axis, length in enumerate(drawn.shape)]
    longest = drawn.shape.index(max(drawn.shape))
    next_to = place[:longest] + [(place[longest] + 1) % drawn.shape[longest]] + place[longest + 1:]
    return drawn.at[tuple(place)].set(low).at[tuple(next_to)].set(top_value)


def setup_inputs(seed: int = 0) -> dict:
    arg_keys = jax.random.split(jax.random.key(seed), 3)
    return {
        "values": draw_values(jax.random.fold_in(arg_keys[2], 71), 0),
        "pattern": touch_ends(jax.random.randint(arg_keys[1], (LR, N_PROW, LC, N_PCOL), 0, 2), jax.random.fold_in(arg_keys[1], 1), 0, 1).astype(jnp.int32),
    }


shift_coef = 5.0

def newton(block, shift):
    width = block.shape[0]
    eye = jnp.eye(width, dtype=block.dtype)
    approx = eye / shift
    for step in range(SWEEPS):
        inner = jnp.dot(block, approx, precision=lax.Precision.HIGHEST)
        approx = jnp.dot(approx, 2.0 * eye - inner, precision=lax.Precision.HIGHEST)
    return approx

def reference(values, pattern):
    nrow = LR * N_PROW
    ncol = LC * N_PCOL
    width = values.shape[4]
    shift = shift_coef * math.sqrt(width)
    grid = values.reshape(nrow, ncol, width, width) * pattern.reshape(nrow, ncol)[:, :, None, None].astype(values.dtype)
    eye = jnp.eye(width, dtype=values.dtype)
    rows_g = jnp.arange(nrow, dtype=jnp.int32)
    cols_g = jnp.arange(ncol, dtype=jnp.int32)
    diag = rows_g[:, None] == cols_g[None, :]
    grid = grid + jnp.where(diag, shift, 0.0).astype(values.dtype)[:, :, None, None] * eye
    for k in range(2):
        inverse = newton(grid[k, k], shift)
        mult = jnp.einsum('rab,be->rae', grid[:, k], inverse, precision=lax.Precision.HIGHEST)
        upper = grid[k]

        def one_row(item):
            row, lrow, index = item
            product = jnp.einsum('ab,cbe->cae', lrow, upper, precision=lax.Precision.HIGHEST)
            trail = (index > k) & (cols_g > k)
            store = (index > k) & (cols_g == k)
            out = jnp.where(trail[:, None, None], row - product, row)
            return jnp.where(store[:, None, None], lrow[None], out)
        grid = lax.map(one_row, (grid, mult, rows_g))
    return grid.reshape(LR, N_PROW, LC, N_PCOL, width, width)
```

```python
import functools
import math

import jax
import jax.numpy as jnp
from jax import lax
from jax.experimental import pallas as pl
from jax.experimental.pallas import tpu as pltpu
from jax.sharding import PartitionSpec as P


SWEEPS = 3

shift_coef = 5.0


def split(x):
    high = x.astype(jnp.bfloat16)
    return high, (x - high.astype(jnp.float32)).astype(jnp.bfloat16)


def dot3(a, b):
    mul = functools.partial(jnp.dot, preferred_element_type=jnp.float32)
    return mul(a[0], b[0]) + mul(a[0], b[1]) + mul(a[1], b[0])


def identity(width):
    row = lax.broadcasted_iota(jnp.int32, (width, width), 0)
    col = lax.broadcasted_iota(jnp.int32, (width, width), 1)
    return jnp.where(row == col, 1.0, 0.0).astype(jnp.float32)


def newton(block, shift, eye):
    error = eye - block * (1.0 / shift)
    approx = (eye + error) * (1.0 / shift)
    for _ in range(1, SWEEPS):
        parts = split(error)
        error = dot3(parts, parts)
        approx = approx + dot3(split(approx), split(error))
    return approx


def pivot_blocks(shift, first, mine, other, out):
    width = mine.shape[1]
    eye = identity(width)
    a00 = jnp.where(first, mine[0], other[0])
    a10 = jnp.where(first, mine[1], other[1])
    a01 = jnp.where(first, other[0], mine[0])
    a11 = jnp.where(first, other[1], mine[1])
    x0 = newton(a00, shift, eye)
    x0s = split(x0)
    a01s = split(a01)
    t1 = dot3(split(a10), x0s)
    z = dot3(x0s, a01s)
    t1s, zs = split(t1), split(z)
    x1 = newton(a11 - dot3(t1s, a01s), shift, eye)
    x1s = split(x1)
    k10 = dot3(x1s, t1s)
    out[0] = x0 + dot3(zs, split(k10))
    out[1] = -dot3(zs, x1s)
    out[2] = -k10
    out[3] = x1
    out[4] = t1
    out[5] = x0


def factor_kernel(shift, plan, place, mine_in, other_in, *refs):
    right, row_one, blocks, upper, pivot, sems, upper_sems = refs[-7:]
    ncols, width = upper.shape[0] // 2, upper.shape[2]
    pcol, core = place[1], place[2]
    near = [pltpu.make_async_copy(mine_in, blocks.at[0], sems.at[0]), pltpu.make_async_copy(other_in, blocks.at[1], sems.at[1])]
    for copy in near:
        copy.start()
    picked_copies(plan, place, refs[:-7], upper, upper_sems, False)
    for copy in near:
        copy.wait()
    pivot_blocks(shift, core == 0, blocks.at[0], blocks.at[1], pivot)
    picked_copies(plan, place, refs[:-7], upper, upper_sems, True)
    w = [split(pivot[n]) for n in range(5)]
    for c in range(ncols):
        cols = slice(c * width, (c + 1) * width)
        u0, u1 = split(upper[c]), split(upper[ncols + c])
        g0 = dot3(w[0], u0) + dot3(w[1], u1)
        g1 = dot3(w[2], u0) + dot3(w[3], u1)
        one = upper[ncols + c] - dot3(w[4], u0)
        if c == 0:
            g0 = jnp.where(pcol == 0, -pivot[5], jnp.where(pcol == 1, -pivot[1], g0))
            g1 = jnp.where(pcol == 0, 0.0, jnp.where(pcol == 1, -pivot[3], g1))
            one = jnp.where(pcol == 0, pivot[4], one)
        row_one[c] = one
        near = split(jnp.where(core == 0, g0, g1))
        far = split(jnp.where(core == 0, g1, g0))
        for n, piece in enumerate((near[0], far[0], near[1], far[1], near[0], far[0])):
            right[n * width:(n + 1) * width, cols] = piece


def update_kernel(sizes, shift, place, pattern, values, mine_a, mine_b, other_a, other_b, right, one, *rest):
    nprow, npcol, half, count, base, ncols, width = sizes
    out, blocks, sides, left, sems, side_sems, out_sems = rest[-7:]
    prow, pcol, core = place[0], place[1], place[2]

    def row0(part):
        return jnp.where(part == 0, core, 1 - core) * half + base

    def fetch(n):
        c, part = n // 2, n % 2
        return pltpu.make_async_copy(values.at[pl.ds(row0(part), count), c], blocks.at[n], sems.at[n])

    def store(n):
        c, part = n // 2, n % 2
        return pltpu.make_async_copy(blocks.at[n], out.at[pl.ds(row0(part), count), c], out_sems.at[n])

    def fetch_all(c):
        fetch(2 * c).start()
        fetch(2 * c + 1).start()

    sources = [pltpu.make_async_copy(ref, sides.at[n], side_sems.at[n]) for n, ref in enumerate((other_b, other_a))]
    for copy in sources:
        copy.start()
    for c in range(min(2, ncols)):
        fetch_all(c)
    for part, (near, far) in enumerate(((mine_a, mine_b), (sides.at[0], sides.at[1]))):
        if part == 1:
            for copy in sources:
                copy.wait()
        near_high, near_low = split(near[...].reshape(count * width, width))
        far_high, far_low = split(far[...].reshape(count * width, width))
        rows = slice(part * count * width, (part + 1) * count * width)
        for k, piece in enumerate((near_high, far_high, near_high, far_high, near_low, far_low)):
            left[rows, k * width:(k + 1) * width] = piece
    for c in range(ncols):
        if c + 2 < ncols:
            fetch_all(c + 2)
        cols = slice(c * width, (c + 1) * width)
        product = jnp.dot(left[...], right[:, cols], preferred_element_type=jnp.float32)
        for part in range(2):
            n = 2 * c + part
            fetch(n).wait()
            first = row0(part)
            for r in range(count):
                keep = pattern[first + r, c].astype(jnp.float32)
                if c == 0:
                    keep = jnp.where((pcol < 2) & ((first + r > 0) | (prow > 0)), 0.0, keep)
                at = (part * count + r) * width
                change = product[at:at + width]
                if base == 0 and r == 0:
                    change = jnp.where((first == 0) & (prow == 0), 0.0, change)
                blocks[n, r] = blocks[n, r] * keep - change
            for r in range(count):
                row_g = (first + r) * nprow + prow

                @pl.when((row_g == c * npcol + pcol) & (row_g != 1))
                def _():
                    blocks[n, r] = blocks[n, r] + shift * identity(width)

            if base == 0:
                @pl.when((first == 0) & (prow == 1))
                def _():
                    blocks[n, 0] = one[c]

            store(n).start()
    for n in range(2 * ncols):
        store(n).wait()


def rows_kernel(sizes, shift, place, pattern, values, whole, *parts):
    npcol, starts = sizes
    prow, pcol = place[0], place[1]
    ncols, width = values.shape[1], values.shape[2]
    for c in range(ncols):
        on = jnp.where(c * npcol + pcol == prow, shift, 0.0)
        block = values[0, c] * pattern[0, c].astype(jnp.float32) + on * identity(width)
        whole[c] = block
        n = max(n for n in range(len(starts)) if starts[n] <= c)
        parts[n][c - starts[n]] = block


def cols_kernel(sizes, shift, place, pattern, near, far, *parts):
    nprow, half, cut = sizes
    prow, pcol, core = place[0], place[1], place[2]
    width = near.shape[2]
    for owner, source, pieces in ((1 - core, far, parts[0:2]), (core, near, parts[2:4])):
        for r in range(half):
            row = owner * half + r
            block = source[r, 0] * pattern[row, 0].astype(jnp.float32)
            if r == 0:
                block = block + jnp.where(row * nprow + prow == pcol, shift, 0.0) * identity(width)
            pieces[r >= cut][r - cut * (r >= cut)] = block


def picked_copies(plan, place, refs, out, sems, wait):
    at = 0
    for n, (entry, start, count, offsets) in enumerate(plan):
        for k, offset in enumerate(offsets):
            source = refs[at + k].at[pl.ds(offset, count)]

            @pl.when(place[entry] == k)
            def _():
                copy = pltpu.make_async_copy(source, out.at[pl.ds(start, count)], sems.at[n])
                copy.wait() if wait else copy.start()
        at += len(offsets)


def pick_kernel(plan, place, *refs):
    for wait in (False, True):
        picked_copies(plan, place, refs[:-2], refs[-2], refs[-1], wait)


def pick_plan(groups):
    start, plan, operands = 0, [], []
    for entry, count, candidates in groups:
        plan.append((entry, start, count, tuple(offset for _, offset in candidates)))
        operands += [array for array, _ in candidates]
        start += count
    return tuple(plan), operands, start


def pick(place, groups):
    plan, operands, total = pick_plan(groups)
    return pl.pallas_call(
        functools.partial(pick_kernel, plan),
        out_shape=jax.ShapeDtypeStruct((total,) + operands[0].shape[1:], jnp.float32),
        in_specs=[pl.BlockSpec(memory_space=pltpu.SMEM)] + [pl.BlockSpec(memory_space=pl.ANY)] * len(operands),
        out_specs=pl.BlockSpec(memory_space=pltpu.VMEM),
        scratch_shapes=[pltpu.SemaphoreType.DMA((len(plan),))],
        name="pick",
    )(place, *operands)


def ring_of(chips):
    return [0] + list(range(1, chips, 2)) + list(range((chips - 1) // 2 * 2, 0, -2))


def choose(index, options):
    out = options[0]
    for n in range(1, len(options)):
        out = jnp.where(index == n, options[n], out)
    return out


def body(values, pattern):
    nrows, ncols, width = values.shape[0], values.shape[2], values.shape[4]
    nprow, npcol = lax.axis_size("prow"), lax.axis_size("pcol")
    chips = npcol // 2
    half = nrows // 2
    cut = half // 2
    prow, pcol = lax.axis_index("prow"), lax.axis_index("pcol")
    core = pcol % 2
    shift = shift_coef * math.sqrt(width)
    vals, pat = values[:, 0, :, 0], pattern[:, 0, :, 0]
    ring = ring_of(chips)
    rings = [ring, [ring[0]] + ring[:0:-1]]
    spot = sum(jnp.where(pcol // 2 == c, jnp.where(core == 0, rings[0].index(c), rings[1].index(c)), 0) for c in range(chips))
    place = jnp.stack([prow, pcol, core, spot]).astype(jnp.int32)
    smem = pl.BlockSpec(memory_space=pltpu.SMEM)
    vmem = pl.BlockSpec(memory_space=pltpu.VMEM)
    array = lambda *shape: jax.ShapeDtypeStruct(shape + (width, width), jnp.float32)
    full = lambda *shape: pl.BlockSpec(shape + (width, width), lambda *_: (0,) * (len(shape) + 2))

    counts = [1, 1, ncols - 2] if ncols > 2 else [1] * ncols
    starts = [sum(counts[:n]) for n in range(len(counts))]
    rows = pl.pallas_call(
        functools.partial(rows_kernel, (npcol, tuple(starts)), shift),
        out_shape=[array(ncols)] + [array(count) for count in counts],
        grid_spec=pltpu.PrefetchScalarGridSpec(
            num_scalar_prefetch=2, grid=(1,),
            in_specs=[full(1, ncols)],
            out_specs=[full(ncols)] + [full(count) for count in counts],
        ),
        name="rows",
    )(place, pat, vals)
    cols = pl.pallas_call(
        functools.partial(cols_kernel, (nprow, half, cut), shift),
        out_shape=[array(cut), array(half - cut)] * 2,
        grid_spec=pltpu.PrefetchScalarGridSpec(
            num_scalar_prefetch=2, grid=(1,),
            in_specs=[
                pl.BlockSpec((half, 1, width, width), lambda _, place, pat: (place[2], 0, 0, 0)),
                pl.BlockSpec((half, 1, width, width), lambda _, place, pat: (1 - place[2], 0, 0, 0)),
            ],
            out_specs=[full(cut), full(half - cut)] * 2,
        ),
        name="cols",
    )(place, pat, vals, vals)

    back = lax.ppermute(rows[0], "prow", [(1, 0)])
    upper0, upper1 = [], []
    for n, (start, count) in enumerate(zip(starts, counts)):
        hops = [rows[1 + n]]
        for hop in range(1, nprow):
            pairs = [(hop - 1, hop)] + ([(hop, hop + 1)] if hop + 1 < nprow else [])
            hops.append(lax.ppermute(hops[-1], "prow", pairs))
        upper0.append((0, count, [(hop, 0) for hop in hops]))
        upper1.append((0, count, [(back, start)] + [(hop, 0) for hop in hops[:-1]]))
    pivots = pick(place, [upper0[0], upper1[0]])

    swap_pairs = [(q, q ^ 1) for q in range(npcol)]
    crossed = []
    for n in range(2):
        crossed.append(lax.ppermute(cols[n], "pcol", swap_pairs))
    sent = [cols[2], crossed[0], cols[3], pivots, crossed[1]]
    got = []
    for chunk in sent:
        hops = [chunk]
        for hop in range(1, chips):
            pairs = [(2 * way[hop - 1] + b, 2 * way[hop] + b) for b, way in enumerate(rings)]
            hops.append(lax.ppermute(hops[-1], "pcol", pairs))
        got.append(choose(spot, hops))
    swapped = []
    for chunk in got:
        swapped.append(lax.ppermute(chunk, "pcol", swap_pairs))

    anywhere = pl.BlockSpec(memory_space=pl.ANY)
    plan, operands, _ = pick_plan(upper0 + upper1)
    right, row_one = pl.pallas_call(
        functools.partial(factor_kernel, shift, plan),
        out_shape=[jax.ShapeDtypeStruct((6 * width, ncols * width), jnp.bfloat16), array(ncols)],
        in_specs=[smem] + [anywhere] * (2 + len(operands)),
        out_specs=[vmem, vmem],
        scratch_shapes=[
            pltpu.VMEM((2, 2, width, width), jnp.float32),
            pltpu.VMEM((2 * ncols, width, width), jnp.float32),
            pltpu.VMEM((6, width, width), jnp.float32),
            pltpu.SemaphoreType.DMA((2,)),
            pltpu.SemaphoreType.DMA((len(plan),)),
        ],
        compiler_params=pltpu.CompilerParams(vmem_limit_bytes=24 * 1024 * 1024),
        name="factor",
    )(place, got[3], swapped[3], *operands)

    out = None
    for base, count, a, b in [(0, cut, 0, 1), (cut, half - cut, 2, 4)]:
        carried = [] if out is None else [out]
        out = pl.pallas_call(
            functools.partial(update_kernel, (nprow, npcol, half, count, base, ncols, width), shift),
            out_shape=jax.ShapeDtypeStruct(vals.shape, jnp.float32),
            in_specs=[smem, smem, anywhere, vmem, vmem, anywhere, anywhere, vmem, vmem] + [anywhere] * len(carried),
            out_specs=anywhere,
            scratch_shapes=[
                pltpu.VMEM((2 * ncols, count, width, width), jnp.float32),
                pltpu.VMEM((2, count, width, width), jnp.float32),
                pltpu.VMEM((2 * count * width, 6 * width), jnp.bfloat16),
                pltpu.SemaphoreType.DMA((2 * ncols,)),
                pltpu.SemaphoreType.DMA((2,)),
                pltpu.SemaphoreType.DMA((2 * ncols,)),
            ],
            input_output_aliases={9: 0} if carried else {},
            compiler_params=pltpu.CompilerParams(vmem_limit_bytes=40 * 1024 * 1024),
        )(place, pat, vals, got[a], got[b], swapped[a], swapped[b], right, row_one, *carried)
    return out[:, None, :, None]


def solution(mesh):
    placed = (P(None, "prow", None, "pcol", None, None), P(None, "prow", None, "pcol"))
    return jax.shard_map(
        body,
        mesh=mesh,
        in_specs=placed,
        out_specs=P(None, "prow", None, "pcol", None, None),
        check_vma=False,
    )
```

```python
import functools
import math

import jax
import jax.numpy as jnp
from jax import lax
from jax.experimental import pallas as pl
from jax.experimental.pallas import tpu as pltpu
from jax.sharding import PartitionSpec as P


SWEEPS = 3

shift_coef = 5.0


def split(x):
    high = x.astype(jnp.bfloat16)
    return high, (x - high.astype(jnp.float32)).astype(jnp.bfloat16)


def dot3(a, b):
    mul = functools.partial(jnp.dot, preferred_element_type=jnp.float32)
    return mul(a[0], b[0]) + mul(a[0], b[1]) + mul(a[1], b[0])


def identity(width):
    row = lax.broadcasted_iota(jnp.int32, (width, width), 0)
    col = lax.broadcasted_iota(jnp.int32, (width, width), 1)
    return jnp.where(row == col, 1.0, 0.0).astype(jnp.float32)


def newton(block, shift, eye):
    error = eye - block * (1.0 / shift)
    approx = (eye + error) * (1.0 / shift)
    for _ in range(1, SWEEPS):
        parts = split(error)
        error = dot3(parts, parts)
        approx = approx + dot3(split(approx), split(error))
    return approx


def pivot_blocks(shift, first, mine, other, out):
    width = mine.shape[1]
    eye = identity(width)
    a00 = jnp.where(first, mine[0], other[0])
    a10 = jnp.where(first, mine[1], other[1])
    a01 = jnp.where(first, other[0], mine[0])
    a11 = jnp.where(first, other[1], mine[1])
    x0 = newton(a00, shift, eye)
    x0s = split(x0)
    a01s = split(a01)
    t1 = dot3(split(a10), x0s)
    z = dot3(x0s, a01s)
    t1s, zs = split(t1), split(z)
    x1 = newton(a11 - dot3(t1s, a01s), shift, eye)
    x1s = split(x1)
    k10 = dot3(x1s, t1s)
    out[0] = x0 + dot3(zs, split(k10))
    out[1] = -dot3(zs, x1s)
    out[2] = -k10
    out[3] = x1
    out[4] = t1
    out[5] = x0


def factor_kernel(shift, plan, place, mine_in, other_in, *refs):
    right, row_one, blocks, upper, pivot, sems, upper_sems = refs[-7:]
    ncols, width = upper.shape[0] // 2, upper.shape[2]
    pcol, core = place[1], place[2]
    near = [pltpu.make_async_copy(mine_in, blocks.at[0], sems.at[0]), pltpu.make_async_copy(other_in, blocks.at[1], sems.at[1])]
    for copy in near:
        copy.start()
    picked_copies(plan, place, refs[:-7], upper, upper_sems, False)
    for copy in near:
        copy.wait()
    pivot_blocks(shift, core == 0, blocks.at[0], blocks.at[1], pivot)
    picked_copies(plan, place, refs[:-7], upper, upper_sems, True)
    w = [split(pivot[n]) for n in range(5)]
    for c in range(ncols):
        cols = slice(c * width, (c + 1) * width)
        u0, u1 = split(upper[c]), split(upper[ncols + c])
        g0 = dot3(w[0], u0) + dot3(w[1], u1)
        g1 = dot3(w[2], u0) + dot3(w[3], u1)
        one = upper[ncols + c] - dot3(w[4], u0)
        if c == 0:
            g0 = jnp.where(pcol == 0, -pivot[5], jnp.where(pcol == 1, -pivot[1], g0))
            g1 = jnp.where(pcol == 0, 0.0, jnp.where(pcol == 1, -pivot[3], g1))
            one = jnp.where(pcol == 0, pivot[4], one)
        row_one[c] = one
        near = split(jnp.where(core == 0, g0, g1))
        far = split(jnp.where(core == 0, g1, g0))
        for n, piece in enumerate((near[0], near[1], near[0], far[0], far[1], far[0])):
            right[n * width:(n + 1) * width, cols] = piece


def update_kernel(sizes, shift, place, pattern, values, mine_a, mine_b, other_a, other_b, right, one, *rest):
    nprow, npcol, half, count, base, ncols, width = sizes
    out, blocks, sides, left, filled, sems, side_sems, out_sems = rest[-8:]
    prow, pcol, core = place[0], place[1], place[2]
    total, ahead = 2 * count, 3

    def row_of(n):
        return jnp.where(n < count, core, 1 - core) * half + base + lax.rem(n, count)

    def fetch(n):
        return pltpu.make_async_copy(values.at[row_of(n)], blocks.at[n], sems.at[n])

    def store(n):
        return pltpu.make_async_copy(blocks.at[n], out.at[row_of(n)], out_sems.at[n])

    sources = [pltpu.make_async_copy(ref, sides.at[n], side_sems.at[n]) for n, ref in enumerate((other_b, other_a))]
    for copy in sources:
        copy.start()
    for n in range(min(ahead, total)):
        fetch(n).start()
    for part, refs in enumerate(((mine_a, mine_b), (sides.at[0], sides.at[1]))):
        if part == 1:
            for copy in sources:
                copy.wait()
        for r in range(count):
            n = part * count + r
            for k, ref in enumerate(refs):
                block = ref[r]
                filled[n, k] = (jnp.max(jnp.abs(block)) > 0).astype(jnp.int32)
                high, low = split(block)
                for m, piece in enumerate((high, high, low)):
                    left[n * width:(n + 1) * width, (3 * k + m) * width:(3 * k + m + 1) * width] = piece

    def step(n, carry):
        @pl.when(n + ahead < total)
        def _():
            fetch(n + ahead).start()

        row = row_of(n)
        row_g = row * nprow + prow
        keep = [pattern[row, c].astype(jnp.float32) for c in range(ncols)]
        keep[0] = jnp.where((pcol < 2) & (row_g > 0), 0.0, keep[0])
        near, far = (filled[n, 0] > 0) & (row_g > 1), (filled[n, 1] > 0) & (row_g > 1)
        rows = pl.ds(pl.multiple_of(n * width, width), width)
        fetch(n).wait()

        def run(inner):
            for c in range(ncols):
                product = jnp.dot(left[rows, inner], right[inner, c * width:(c + 1) * width], preferred_element_type=jnp.float32)
                blocks[n, c] = blocks[n, c] * keep[c] - product

        @pl.when(near & far)
        def _():
            run(slice(0, 6 * width))

        @pl.when(near & jnp.logical_not(far))
        def _():
            run(slice(0, 3 * width))

        @pl.when(far & jnp.logical_not(near))
        def _():
            run(slice(3 * width, 6 * width))

        @pl.when(jnp.logical_not(near | far))
        def _():
            for c in range(ncols):
                blocks[n, c] = blocks[n, c] * keep[c]

        at = jnp.minimum(row_g // npcol, ncols - 1)

        @pl.when((row_g == at * npcol + pcol) & ((row_g > 1) | (row_g == 0)))
        def _():
            blocks[n, at] = blocks[n, at] + shift * identity(width)

        if base == 0:
            @pl.when(row_g == 1)
            def _():
                for c in range(ncols):
                    blocks[n, c] = one[c]

        store(n).start()
        return carry

    lax.fori_loop(0, total, step, 0)
    for n in range(total):
        store(n).wait()


def rows_kernel(sizes, shift, place, pattern, values, whole, *parts):
    npcol, starts = sizes
    prow, pcol = place[0], place[1]
    ncols, width = values.shape[1], values.shape[2]
    for c in range(1, ncols):
        on = jnp.where(c * npcol + pcol == prow, shift, 0.0)
        block = values[0, c] * pattern[0, c].astype(jnp.float32) + on * identity(width)
        whole[c - 1] = block
        n = max(n for n in range(len(starts)) if starts[n] <= c)
        parts[n - 1][c - starts[n]] = block


def cols_kernel(sizes, shift, place, pattern, near, far, *parts):
    nprow, half, cut = sizes
    prow, pcol, core = place[0], place[1], place[2]
    width = near.shape[2]
    for owner, source, pieces in ((1 - core, far, parts[0:2]), (core, near, parts[2:4])):
        for r in range(half):
            row = owner * half + r
            block = source[r, 0] * pattern[row, 0].astype(jnp.float32)
            if r == 0:
                block = block + jnp.where(row * nprow + prow == pcol, shift, 0.0) * identity(width)
            pieces[r >= cut][r - cut * (r >= cut)] = block


def picked_copies(plan, place, refs, out, sems, wait):
    at = 0
    for n, (entry, start, count, offsets) in enumerate(plan):
        for k, offset in enumerate(offsets):
            source = refs[at + k].at[pl.ds(offset, count)]

            @pl.when(place[entry] == k)
            def _():
                copy = pltpu.make_async_copy(source, out.at[pl.ds(start, count)], sems.at[n])
                copy.wait() if wait else copy.start()
        at += len(offsets)


def pick_kernel(plan, place, *refs):
    for wait in (False, True):
        picked_copies(plan, place, refs[:-2], refs[-2], refs[-1], wait)


def pick_plan(groups):
    start, plan, operands = 0, [], []
    for entry, count, candidates in groups:
        plan.append((entry, start, count, tuple(offset for _, offset in candidates)))
        operands += [array for array, _ in candidates]
        start += count
    return tuple(plan), operands, start


def pick(place, groups):
    plan, operands, total = pick_plan(groups)
    return pl.pallas_call(
        functools.partial(pick_kernel, plan),
        out_shape=jax.ShapeDtypeStruct((total,) + operands[0].shape[1:], jnp.float32),
        in_specs=[pl.BlockSpec(memory_space=pltpu.SMEM)] + [pl.BlockSpec(memory_space=pl.ANY)] * len(operands),
        out_specs=pl.BlockSpec(memory_space=pltpu.VMEM),
        scratch_shapes=[pltpu.SemaphoreType.DMA((len(plan),))],
        name="pick",
    )(place, *operands)


def ring_of(chips):
    return [0] + list(range(1, chips, 2)) + list(range((chips - 1) // 2 * 2, 0, -2))


def choose(index, options):
    out = options[0]
    for n in range(1, len(options)):
        out = jnp.where(index == n, options[n], out)
    return out


def body(values, pattern):
    nrows, ncols, width = values.shape[0], values.shape[2], values.shape[4]
    nprow, npcol = lax.axis_size("prow"), lax.axis_size("pcol")
    chips = npcol // 2
    half = nrows // 2
    cut = half // 2
    prow, pcol = lax.axis_index("prow"), lax.axis_index("pcol")
    core = pcol % 2
    shift = shift_coef * math.sqrt(width)
    vals, pat = values[:, 0, :, 0], pattern[:, 0, :, 0]
    ring = ring_of(chips)
    rings = [ring, [ring[0]] + ring[:0:-1]]
    spot = sum(jnp.where(pcol // 2 == c, jnp.where(core == 0, rings[0].index(c), rings[1].index(c)), 0) for c in range(chips))
    place = jnp.stack([prow, pcol, core, spot]).astype(jnp.int32)
    smem = pl.BlockSpec(memory_space=pltpu.SMEM)
    vmem = pl.BlockSpec(memory_space=pltpu.VMEM)
    array = lambda *shape: jax.ShapeDtypeStruct(shape + (width, width), jnp.float32)
    full = lambda *shape: pl.BlockSpec(shape + (width, width), lambda *_: (0,) * (len(shape) + 2))

    counts = [1, 1, ncols - 2] if ncols > 2 else [1] * ncols
    starts = [sum(counts[:n]) for n in range(len(counts))]
    rows = pl.pallas_call(
        functools.partial(rows_kernel, (npcol, tuple(starts)), shift),
        out_shape=[array(ncols - 1)] + [array(count) for count in counts[1:]],
        grid_spec=pltpu.PrefetchScalarGridSpec(
            num_scalar_prefetch=2, grid=(1,),
            in_specs=[full(1, ncols)],
            out_specs=[full(ncols - 1)] + [full(count) for count in counts[1:]],
        ),
        name="rows",
    )(place, pat, vals)
    on = jnp.where(prow == pcol, shift, 0.0)
    first_row = vals[0, 0:1] * pat[0, 0].astype(jnp.float32) + on * jnp.eye(width, dtype=jnp.float32)
    cols = pl.pallas_call(
        functools.partial(cols_kernel, (nprow, half, cut), shift),
        out_shape=[array(cut), array(half - cut)] * 2,
        grid_spec=pltpu.PrefetchScalarGridSpec(
            num_scalar_prefetch=2, grid=(1,),
            in_specs=[
                pl.BlockSpec((half, 1, width, width), lambda _, place, pat: (place[2], 0, 0, 0)),
                pl.BlockSpec((half, 1, width, width), lambda _, place, pat: (1 - place[2], 0, 0, 0)),
            ],
            out_specs=[full(cut), full(half - cut)] * 2,
        ),
        name="cols",
    )(place, pat, vals, vals)

    back0 = lax.ppermute(first_row, "prow", [(1, 0)])
    back1 = lax.ppermute(rows[0], "prow", [(1, 0)])
    upper0, upper1 = [], []
    for n, (start, count) in enumerate(zip(starts, counts)):
        hops = [rows[n] if n else first_row]
        for hop in range(1, nprow):
            pairs = [(hop - 1, hop)] + ([(hop, hop + 1)] if hop + 1 < nprow else [])
            hops.append(lax.ppermute(hops[-1], "prow", pairs))
        upper0.append((0, count, [(hop, 0) for hop in hops]))
        upper1.append((0, count, [(back1, start - 1) if n else (back0, 0)] + [(hop, 0) for hop in hops[:-1]]))
    pivots = pick(place, [upper0[0], upper1[0]])

    swap_pairs = [(q, q ^ 1) for q in range(npcol)]
    crossed = []
    for n in range(2):
        crossed.append(lax.ppermute(cols[n], "pcol", swap_pairs))
    sent = [cols[2], crossed[0], cols[3], pivots, crossed[1]]
    got = []
    for chunk in sent:
        hops = [chunk]
        for hop in range(1, chips):
            pairs = [(2 * way[hop - 1] + b, 2 * way[hop] + b) for b, way in enumerate(rings)]
            hops.append(lax.ppermute(hops[-1], "pcol", pairs))
        got.append(choose(spot, hops))
    swapped = []
    for chunk in got:
        swapped.append(lax.ppermute(chunk, "pcol", swap_pairs))

    anywhere = pl.BlockSpec(memory_space=pl.ANY)
    plan, operands, _ = pick_plan(upper0 + upper1)
    right, row_one = pl.pallas_call(
        functools.partial(factor_kernel, shift, plan),
        out_shape=[jax.ShapeDtypeStruct((6 * width, ncols * width), jnp.bfloat16), array(ncols)],
        in_specs=[smem] + [anywhere] * (2 + len(operands)),
        out_specs=[vmem, vmem],
        scratch_shapes=[
            pltpu.VMEM((2, 2, width, width), jnp.float32),
            pltpu.VMEM((2 * ncols, width, width), jnp.float32),
            pltpu.VMEM((6, width, width), jnp.float32),
            pltpu.SemaphoreType.DMA((2,)),
            pltpu.SemaphoreType.DMA((len(plan),)),
        ],
        compiler_params=pltpu.CompilerParams(vmem_limit_bytes=24 * 1024 * 1024),
        name="factor",
    )(place, got[3], swapped[3], *operands)

    out = None
    for base, count, a, b in [(0, cut, 0, 1), (cut, half - cut, 2, 4)]:
        carried = [] if out is None else [out]
        out = pl.pallas_call(
            functools.partial(update_kernel, (nprow, npcol, half, count, base, ncols, width), shift),
            out_shape=jax.ShapeDtypeStruct(vals.shape, jnp.float32),
            in_specs=[smem, smem, anywhere, vmem, vmem, anywhere, anywhere, vmem, vmem] + [anywhere] * len(carried),
            out_specs=anywhere,
            scratch_shapes=[
                pltpu.VMEM((2 * count, ncols, width, width), jnp.float32),
                pltpu.VMEM((2, count, width, width), jnp.float32),
                pltpu.VMEM((2 * count * width, 6 * width), jnp.bfloat16),
                pltpu.SMEM((2 * count, 2), jnp.int32),
                pltpu.SemaphoreType.DMA((2 * count,)),
                pltpu.SemaphoreType.DMA((2,)),
                pltpu.SemaphoreType.DMA((2 * count,)),
            ],
            input_output_aliases={9: 0} if carried else {},
            compiler_params=pltpu.CompilerParams(vmem_limit_bytes=40 * 1024 * 1024),
        )(place, pat, vals, got[a], got[b], swapped[a], swapped[b], right, row_one, *carried)
    return out[:, None, :, None]


def solution(mesh):
    placed = (P(None, "prow", None, "pcol", None, None), P(None, "prow", None, "pcol"))
    return jax.shard_map(
        body,
        mesh=mesh,
        in_specs=placed,
        out_specs=P(None, "prow", None, "pcol", None, None),
        check_vma=False,
    )
```

```python
import functools
import math

import jax
import jax.numpy as jnp
from jax import lax
from jax.experimental import pallas as pl
from jax.experimental.pallas import tpu as pltpu
from jax.sharding import PartitionSpec as P


SWEEPS = 3

shift_coef = 5.0


def split(x):
    high = x.astype(jnp.bfloat16)
    return high, (x - high.astype(jnp.float32)).astype(jnp.bfloat16)


def dot3(a, b):
    mul = functools.partial(jnp.dot, preferred_element_type=jnp.float32)
    return mul(a[0], b[0]) + mul(a[0], b[1]) + mul(a[1], b[0])


def identity(width):
    row = lax.broadcasted_iota(jnp.int32, (width, width), 0)
    col = lax.broadcasted_iota(jnp.int32, (width, width), 1)
    return jnp.where(row == col, 1.0, 0.0).astype(jnp.float32)


def newton(block, shift, eye):
    error = eye - block * (1.0 / shift)
    approx = (eye + error) * (1.0 / shift)
    for _ in range(1, SWEEPS):
        parts = split(error)
        error = dot3(parts, parts)
        approx = approx + dot3(split(approx), split(error))
    return approx


def pivot_blocks(shift, first, mine, other, out):
    width = mine.shape[1]
    eye = identity(width)
    a00 = jnp.where(first, mine[0], other[0])
    a10 = jnp.where(first, mine[1], other[1])
    a01 = jnp.where(first, other[0], mine[0])
    a11 = jnp.where(first, other[1], mine[1])
    x0 = newton(a00, shift, eye)
    x0s = split(x0)
    a01s = split(a01)
    t1 = dot3(split(a10), x0s)
    z = dot3(x0s, a01s)
    t1s, zs = split(t1), split(z)
    x1 = newton(a11 - dot3(t1s, a01s), shift, eye)
    x1s = split(x1)
    k10 = dot3(x1s, t1s)
    out[0] = x0 + dot3(zs, split(k10))
    out[1] = -dot3(zs, x1s)
    out[2] = -k10
    out[3] = x1
    out[4] = t1
    out[5] = x0


def factor_kernel(shift, plan, place, mine_in, other_in, *refs):
    right, row_one, blocks, upper, pivot, sems, upper_sems = refs[-7:]
    ncols, width = upper.shape[0] // 2, upper.shape[2]
    pcol, core = place[1], place[2]
    near = [pltpu.make_async_copy(mine_in, blocks.at[0], sems.at[0]), pltpu.make_async_copy(other_in, blocks.at[1], sems.at[1])]
    for copy in near:
        copy.start()
    picked_copies(plan, place, refs[:-7], upper, upper_sems, False)
    for copy in near:
        copy.wait()
    pivot_blocks(shift, core == 0, blocks.at[0], blocks.at[1], pivot)
    picked_copies(plan, place, refs[:-7], upper, upper_sems, True)
    w = [split(pivot[n]) for n in range(5)]
    for c in range(ncols):
        cols = slice(c * width, (c + 1) * width)
        u0, u1 = split(upper[c]), split(upper[ncols + c])
        g0 = dot3(w[0], u0) + dot3(w[1], u1)
        g1 = dot3(w[2], u0) + dot3(w[3], u1)
        one = upper[ncols + c] - dot3(w[4], u0)
        if c == 0:
            g0 = jnp.where(pcol == 0, -pivot[5], jnp.where(pcol == 1, -pivot[1], g0))
            g1 = jnp.where(pcol == 0, 0.0, jnp.where(pcol == 1, -pivot[3], g1))
            one = jnp.where(pcol == 0, pivot[4], one)
        row_one[c] = one
        near = split(jnp.where(core == 0, g0, g1))
        far = split(jnp.where(core == 0, g1, g0))
        for n, piece in enumerate((near[0], near[1], near[0], far[0], far[1], far[0])):
            right[n * width:(n + 1) * width, cols] = piece


def update_kernel(sizes, shift, place, pattern, values, mine_a, mine_b, other_a, other_b, right, one, *rest):
    nprow, npcol, half, count, base, ncols, width = sizes
    out, blocks, sides, left, filled, sems, side_sems, out_sems = rest[-8:]
    prow, pcol, core = place[0], place[1], place[2]
    total, ahead = 2 * count, 3

    def row_of(n):
        return jnp.where(n < count, core, 1 - core) * half + base + lax.rem(n, count)

    def fetch(n):
        return pltpu.make_async_copy(values.at[row_of(n)], blocks.at[n], sems.at[n])

    def store(n):
        return pltpu.make_async_copy(blocks.at[n], out.at[row_of(n)], out_sems.at[n])

    sources = [pltpu.make_async_copy(ref, sides.at[n], side_sems.at[n]) for n, ref in enumerate((other_b, other_a))]
    for copy in sources:
        copy.start()
    for n in range(min(ahead, total)):
        fetch(n).start()
    for part, refs in enumerate(((mine_a, mine_b), (sides.at[0], sides.at[1]))):
        if part == 1:
            for copy in sources:
                copy.wait()
        for r in range(count):
            n = part * count + r
            for k, ref in enumerate(refs):
                block = ref[r]
                filled[n, k] = (jnp.max(jnp.abs(block)) > 0).astype(jnp.int32)
                high, low = split(block)
                for m, piece in enumerate((high, high, low)):
                    left[n * width:(n + 1) * width, (3 * k + m) * width:(3 * k + m + 1) * width] = piece

    def step(n, carry):
        @pl.when(n + ahead < total)
        def _():
            fetch(n + ahead).start()

        row = row_of(n)
        row_g = row * nprow + prow
        keep = [pattern[row, c].astype(jnp.float32) for c in range(ncols)]
        keep[0] = jnp.where((pcol < 2) & (row_g > 0), 0.0, keep[0])
        near, far = (filled[n, 0] > 0) & (row_g > 1), (filled[n, 1] > 0) & (row_g > 1)
        rows = pl.ds(pl.multiple_of(n * width, width), width)
        fetch(n).wait()

        def run(inner):
            for c in range(ncols):
                product = jnp.dot(left[rows, inner], right[inner, c * width:(c + 1) * width], preferred_element_type=jnp.float32)
                blocks[n, c] = blocks[n, c] * keep[c] - product

        @pl.when(near & far)
        def _():
            run(slice(0, 6 * width))

        @pl.when(near & jnp.logical_not(far))
        def _():
            run(slice(0, 3 * width))

        @pl.when(far & jnp.logical_not(near))
        def _():
            run(slice(3 * width, 6 * width))

        @pl.when(jnp.logical_not(near | far))
        def _():
            for c in range(ncols):
                blocks[n, c] = blocks[n, c] * keep[c]

        at = jnp.minimum(row_g // npcol, ncols - 1)

        @pl.when((row_g == at * npcol + pcol) & ((row_g > 1) | (row_g == 0)))
        def _():
            blocks[n, at] = blocks[n, at] + shift * identity(width)

        if base == 0:
            @pl.when(row_g == 1)
            def _():
                for c in range(ncols):
                    blocks[n, c] = one[c]

        store(n).start()
        return carry

    lax.fori_loop(0, total, step, 0)
    for n in range(total):
        store(n).wait()


def rows_kernel(npcol, shift, place, pattern, values, out):
    prow, pcol = place[0], place[1]
    ncols, width = values.shape[1], values.shape[2]
    for c in range(1, ncols):
        on = jnp.where(c * npcol + pcol == prow, shift, 0.0)
        out[c - 1] = values[0, c] * pattern[0, c].astype(jnp.float32) + on * identity(width)


def cols_kernel(sizes, shift, place, pattern, near, far, *parts):
    nprow, half, cut = sizes
    prow, pcol, core = place[0], place[1], place[2]
    width = near.shape[2]
    for owner, source, pieces in ((1 - core, far, parts[0:2]), (core, near, parts[2:4])):
        for r in range(half):
            row = owner * half + r
            block = source[r, 0] * pattern[row, 0].astype(jnp.float32)
            if r == 0:
                block = block + jnp.where(row * nprow + prow == pcol, shift, 0.0) * identity(width)
            pieces[r >= cut][r - cut * (r >= cut)] = block


def picked_copies(plan, place, refs, out, sems, wait):
    at = 0
    for n, (entry, start, count, offsets) in enumerate(plan):
        for k, offset in enumerate(offsets):
            source = refs[at + k].at[pl.ds(offset, count)]

            @pl.when(place[entry] == k)
            def _():
                copy = pltpu.make_async_copy(source, out.at[pl.ds(start, count)], sems.at[n])
                copy.wait() if wait else copy.start()
        at += len(offsets)


def pick_kernel(plan, place, *refs):
    for wait in (False, True):
        picked_copies(plan, place, refs[:-2], refs[-2], refs[-1], wait)


def pick_plan(groups):
    start, plan, operands = 0, [], []
    for entry, count, candidates in groups:
        plan.append((entry, start, count, tuple(offset for _, offset in candidates)))
        operands += [array for array, _ in candidates]
        start += count
    return tuple(plan), operands, start


def pick(place, groups):
    plan, operands, total = pick_plan(groups)
    return pl.pallas_call(
        functools.partial(pick_kernel, plan),
        out_shape=jax.ShapeDtypeStruct((total,) + operands[0].shape[1:], jnp.float32),
        in_specs=[pl.BlockSpec(memory_space=pltpu.SMEM)] + [pl.BlockSpec(memory_space=pl.ANY)] * len(operands),
        out_specs=pl.BlockSpec(memory_space=pltpu.VMEM),
        scratch_shapes=[pltpu.SemaphoreType.DMA((len(plan),))],
        name="pick",
    )(place, *operands)


def ring_of(chips):
    return [0] + list(range(1, chips, 2)) + list(range((chips - 1) // 2 * 2, 0, -2))


def choose(index, options):
    out = options[0]
    for n in range(1, len(options)):
        out = jnp.where(index == n, options[n], out)
    return out


def body(values, pattern):
    nrows, ncols, width = values.shape[0], values.shape[2], values.shape[4]
    nprow, npcol = lax.axis_size("prow"), lax.axis_size("pcol")
    chips = npcol // 2
    half = nrows // 2
    cut = half // 2
    prow, pcol = lax.axis_index("prow"), lax.axis_index("pcol")
    core = pcol % 2
    shift = shift_coef * math.sqrt(width)
    vals, pat = values[:, 0, :, 0], pattern[:, 0, :, 0]
    ring = ring_of(chips)
    rings = [ring, [ring[0]] + ring[:0:-1]]
    spot = sum(jnp.where(pcol // 2 == c, jnp.where(core == 0, rings[0].index(c), rings[1].index(c)), 0) for c in range(chips))
    place = jnp.stack([prow, pcol, core, spot]).astype(jnp.int32)
    smem = pl.BlockSpec(memory_space=pltpu.SMEM)
    vmem = pl.BlockSpec(memory_space=pltpu.VMEM)
    array = lambda *shape: jax.ShapeDtypeStruct(shape + (width, width), jnp.float32)
    full = lambda *shape: pl.BlockSpec(shape + (width, width), lambda *_: (0,) * (len(shape) + 2))

    counts = [1, ncols - 1]
    starts = [sum(counts[:n]) for n in range(len(counts))]
    rows = pl.pallas_call(
        functools.partial(rows_kernel, npcol, shift),
        out_shape=[array(ncols - 1)],
        grid_spec=pltpu.PrefetchScalarGridSpec(
            num_scalar_prefetch=2, grid=(1,),
            in_specs=[full(1, ncols)],
            out_specs=[full(ncols - 1)],
        ),
        name="rows",
    )(place, pat, vals)
    on = jnp.where(prow == pcol, shift, 0.0)
    first_row = vals[0, 0:1] * pat[0, 0].astype(jnp.float32) + on * jnp.eye(width, dtype=jnp.float32)
    cols = pl.pallas_call(
        functools.partial(cols_kernel, (nprow, half, cut), shift),
        out_shape=[array(cut), array(half - cut)] * 2,
        grid_spec=pltpu.PrefetchScalarGridSpec(
            num_scalar_prefetch=2, grid=(1,),
            in_specs=[
                pl.BlockSpec((half, 1, width, width), lambda _, place, pat: (place[2], 0, 0, 0)),
                pl.BlockSpec((half, 1, width, width), lambda _, place, pat: (1 - place[2], 0, 0, 0)),
            ],
            out_specs=[full(cut), full(half - cut)] * 2,
        ),
        name="cols",
    )(place, pat, vals, vals)

    back0 = lax.ppermute(first_row, "prow", [(1, 0)])
    back1 = lax.ppermute(rows[0], "prow", [(1, 0)])
    upper0, upper1 = [], []
    for n, (start, count) in enumerate(zip(starts, counts)):
        hops = [rows[0] if n else first_row]
        for hop in range(1, nprow):
            pairs = [(hop - 1, hop)] + ([(hop, hop + 1)] if hop + 1 < nprow else [])
            hops.append(lax.ppermute(hops[-1], "prow", pairs))
        upper0.append((0, count, [(hop, 0) for hop in hops]))
        upper1.append((0, count, [(back1, start - 1) if n else (back0, 0)] + [(hop, 0) for hop in hops[:-1]]))
    pivots = pick(place, [upper0[0], upper1[0]])

    swap_pairs = [(q, q ^ 1) for q in range(npcol)]
    crossed = []
    for n in range(2):
        crossed.append(lax.ppermute(cols[n], "pcol", swap_pairs))
    sent = [cols[2], crossed[0], cols[3], pivots, crossed[1]]
    got = []
    for chunk in sent:
        hops = [chunk]
        for hop in range(1, chips):
            pairs = [(2 * way[hop - 1] + b, 2 * way[hop] + b) for b, way in enumerate(rings)]
            hops.append(lax.ppermute(hops[-1], "pcol", pairs))
        got.append(choose(spot, hops))
    swapped = []
    for chunk in got:
        swapped.append(lax.ppermute(chunk, "pcol", swap_pairs))

    anywhere = pl.BlockSpec(memory_space=pl.ANY)
    plan, operands, _ = pick_plan(upper0 + upper1)
    right, row_one = pl.pallas_call(
        functools.partial(factor_kernel, shift, plan),
        out_shape=[jax.ShapeDtypeStruct((6 * width, ncols * width), jnp.bfloat16), array(ncols)],
        in_specs=[smem] + [anywhere] * (2 + len(operands)),
        out_specs=[vmem, vmem],
        scratch_shapes=[
            pltpu.VMEM((2, 2, width, width), jnp.float32),
            pltpu.VMEM((2 * ncols, width, width), jnp.float32),
            pltpu.VMEM((6, width, width), jnp.float32),
            pltpu.SemaphoreType.DMA((2,)),
            pltpu.SemaphoreType.DMA((len(plan),)),
        ],
        compiler_params=pltpu.CompilerParams(vmem_limit_bytes=24 * 1024 * 1024),
        name="factor",
    )(place, got[3], swapped[3], *operands)

    out = None
    for base, count, a, b in [(0, cut, 0, 1), (cut, half - cut, 2, 4)]:
        carried = [] if out is None else [out]
        out = pl.pallas_call(
            functools.partial(update_kernel, (nprow, npcol, half, count, base, ncols, width), shift),
            out_shape=jax.ShapeDtypeStruct(vals.shape, jnp.float32),
            in_specs=[smem, smem, anywhere, vmem, vmem, anywhere, anywhere, vmem, vmem] + [anywhere] * len(carried),
            out_specs=anywhere,
            scratch_shapes=[
                pltpu.VMEM((2 * count, ncols, width, width), jnp.float32),
                pltpu.VMEM((2, count, width, width), jnp.float32),
                pltpu.VMEM((2 * count * width, 6 * width), jnp.bfloat16),
                pltpu.SMEM((2 * count, 2), jnp.int32),
                pltpu.SemaphoreType.DMA((2 * count,)),
                pltpu.SemaphoreType.DMA((2,)),
                pltpu.SemaphoreType.DMA((2 * count,)),
            ],
            input_output_aliases={9: 0} if carried else {},
            compiler_params=pltpu.CompilerParams(vmem_limit_bytes=40 * 1024 * 1024),
        )(place, pat, vals, got[a], got[b], swapped[a], swapped[b], right, row_one, *carried)
    return out[:, None, :, None]


def solution(mesh):
    placed = (P(None, "prow", None, "pcol", None, None), P(None, "prow", None, "pcol"))
    return jax.shard_map(
        body,
        mesh=mesh,
        in_specs=placed,
        out_specs=P(None, "prow", None, "pcol", None, None),
        check_vma=False,
    )
```
